32 devices in a mesh: enc: 8 (over z, x), tp: 4 (over y, core).
Axes of the slice: x: 2, y: 2, z: 4, core: 2. Of those that a mesh axis runs over, the one named last changes fastest.
Arguments:
- grad_rows: bfloat16 [3072, 8192], P('enc', 'tp'), may hold values from -6 to 6
- features: bfloat16 [3072, 1280], P('enc'), may hold values from -6 to 6
- block_in: bfloat16 [3072, 1280], P('enc', 'tp'), may hold values from -6 to 6
- patch_counts: int32 [8, 3], replicated, may hold values from 32 to 128, as said below
- owner: int32 [8, 3], replicated, may hold values from 0 to 7, as said below
- ln1_gain: float32 [1280], replicated, may hold values from 0.5 to 1.5
- w_qkv: bfloat16 [1280, 16, 240], P(None, 'tp')
- w_out: bfloat16 [1280, 1280], P('tp'), may hold values from -0.15625 to 0.15625
- w_proj: bfloat16 [1280, 8192], P(None, 'tp'), may hold values from -0.15625 to 0.15625
Outputs:
- grad_input: bfloat16 [3072, 1280], P('enc', 'tp')
- grad_proj: float32 [1280, 8192], P('enc', 'tp')
- grad_qkv: float32 [1280, 16, 240], P('enc', 'tp')
- grad_out: float32 [1280, 1280], P('tp', 'enc')
- grad_ln1: float32 [1280], P('enc')
The draws below stay inside these ranges and needn't reach their ends.
Inputs may be any that keep to these rules, and one draw needn't show every extreme that they name: `patch_counts`: some image has exactly 128 live rows and some exactly 32. `owner`: each encoder device receives exactly 3 images, never two from the same block.
All inputs are finite; a program needn't handle non-finite values.
Results may differ from the reference program's by a relative error of at most 0.033.
Values may be sent and summed in bfloat16 or wider, within the bound.
A program may use at most 64 MiB of HBM per device.

```python
import math
import jax
import jax.numpy as jnp
from jax import lax

D_LLM = 8192
D_VIT = 1280
HEADS = 16
HEAD_DIM = 80
TILE = 128
IMG_GROUP = 3
ROWS_DEV = 384
ROWS_ALL = 3072
N_ENC = 8
N_TP = 4


def image_plan(key):
    count_key, first_key, second_key, third_key = jax.random.split(jax.random.fold_in(key, 31), 4)
    counts = jax.random.randint(count_key, (N_ENC, IMG_GROUP), TILE // 4, TILE + 1).astype(jnp.int32)
    counts = counts.at[0, 0].set(TILE).at[N_ENC - 1, IMG_GROUP - 1].set(TILE // 4)
    targets = jax.random.permutation(first_key, N_ENC).astype(jnp.int32)
    starts = jax.random.permutation(second_key, N_ENC).astype(jnp.int32)
    offsets = jax.random.permutation(third_key, N_ENC).astype(jnp.int32)[:IMG_GROUP]
    positions = (starts[:, None] + offsets[None, :]) % N_ENC
    owners = jnp.take(targets, positions.reshape(-1)).reshape(N_ENC, IMG_GROUP)
    return (counts, owners.astype(jnp.int32))


def draw_patch_counts(key, part):
    return image_plan(key)[0]


def draw_owner(key, part):
    return image_plan(key)[1]


def draw_w_qkv(key, part):
    gaussian = jax.random.normal(jax.random.fold_in(key, 5), (D_VIT, HEADS, 3 * HEAD_DIM), jnp.float32) / math.sqrt(D_VIT)
    return gaussian.astype(jnp.bfloat16)


def block_levels(key, dims, cuts, smallest, top_value):
    def one(axis_at, blocks):
        heights = jax.random.uniform(jax.random.fold_in(jax.random.fold_in(key, 6), axis_at), (blocks,), jnp.float32, smallest / len(cuts), top_value / len(cuts))
        return jnp.repeat(jnp.exp(heights), dims[axis_at] // blocks).reshape((-1,) + (1,) * (len(dims) - axis_at - 1))

    factor_of = one(*cuts[0])
    for cut in cuts[1:]:
        factor_of = factor_of * one(*cut)
    return factor_of


def scatter_about(stream_key, dims, width, most, cuts=(), kind=jnp.bfloat16):
    entries = width * jax.random.normal(stream_key, dims, jnp.float32)
    if cuts:
        entries = entries * block_levels(stream_key, dims, cuts, -0.22, 0.18)
    return jnp.clip(entries, -most, most).astype(kind)


def setup_inputs(seed: int = 0) -> dict:
    keys = jax.random.split(jax.random.key(seed), 10)
    grad_rows = scatter_about(keys[0], (ROWS_ALL, D_LLM), 1.0, 6.0, ((0, 8), (1, 4)))
    features = scatter_about(keys[1], (ROWS_ALL, D_VIT), 1.0, 6.0, ((0, 8),))
    block_in = scatter_about(keys[2], (ROWS_ALL, D_VIT), 1.0, 6.0, ((0, 8), (1, 4)))
    patch_counts = draw_patch_counts(jax.random.fold_in(keys[9], 71), 0)
    owner = draw_owner(jax.random.fold_in(keys[9], 71), 0)
    ln1_gain = jnp.clip(1.0 + 0.1 * jax.random.normal(keys[5], (D_VIT,), jnp.float32), 0.5, 1.5)
    w_qkv = draw_w_qkv(jax.random.fold_in(keys[9], 71), 0)
    w_out = scatter_about(keys[7], (D_VIT, D_VIT), D_VIT ** -0.5, 0.15625, ((0, 4),))
    w_proj = scatter_about(keys[8], (D_VIT, D_LLM), D_VIT ** -0.5, 0.15625, ((1, 4),))
    return {"grad_rows": grad_rows, "features": features, "block_in": block_in, "patch_counts": patch_counts, "owner": owner, "ln1_gain": ln1_gain, "w_qkv": w_qkv, "w_out": w_out, "w_proj": w_proj}


EPSILON = 1e-05

def chop(values):
    return lax.optimization_barrier(values.astype(jnp.bfloat16)).astype(jnp.float32)

def normalize(values):
    centred = values - lax.optimization_barrier(jnp.mean(values, axis=-1, keepdims=True))
    variance = lax.optimization_barrier(jnp.mean(centred * centred, axis=-1, keepdims=True))
    inverse = lax.rsqrt(variance + EPSILON)
    return (centred * inverse, inverse)

def norm_back(incoming, normed, inverse, gain):
    scaled = incoming * gain
    inner_mean = lax.optimization_barrier(jnp.mean(scaled * normed, axis=-1, keepdims=True))
    outgoing = inverse * (scaled - lax.optimization_barrier(jnp.mean(scaled, axis=-1, keepdims=True)) - normed * inner_mean)
    return (outgoing, lax.optimization_barrier(jnp.sum(incoming * normed, axis=0)))

def block_backward(block_x, upstream_f, live, ln1_gain, w_qkv, w_out):
    rows_here = block_x.shape[0]
    normed1, inverse1 = normalize(block_x.astype(jnp.float32))
    normed_in = (normed1 * ln1_gain).astype(jnp.bfloat16)
    qkv_flat = w_qkv.reshape(D_VIT, HEADS * 3 * HEAD_DIM)
    packed = jnp.dot(normed_in, qkv_flat, preferred_element_type=jnp.float32).astype(jnp.bfloat16)
    packed = packed.reshape(IMG_GROUP, TILE, HEADS, 3, HEAD_DIM)
    queries = packed[:, :, :, 0, :].astype(jnp.float32)
    keys_part = packed[:, :, :, 1, :].astype(jnp.float32)
    values_part = packed[:, :, :, 2, :].astype(jnp.float32)
    scaling = 1.0 / HEAD_DIM ** 0.5
    scores = jnp.einsum('gqhd,gkhd->ghqk', queries, keys_part) * scaling
    same_kind = (live[:, :, None] == live[:, None, :])[:, None]
    scores = jnp.where(same_kind, scores, -1e+30)
    row_max = lax.optimization_barrier(jnp.max(scores, axis=-1, keepdims=True))
    exp_terms = jnp.exp(scores - row_max)
    probability = exp_terms / lax.optimization_barrier(jnp.sum(exp_terms, axis=-1, keepdims=True))
    prob_low = probability.astype(jnp.bfloat16)
    mixed = jnp.einsum('ghqk,gkhd->gqhd', prob_low.astype(jnp.float32), values_part).astype(jnp.bfloat16)
    mixed = mixed.reshape(rows_here, HEADS * HEAD_DIM)
    middle_b = upstream_f.astype(jnp.bfloat16)
    out_term = jnp.dot(mixed.T, middle_b, preferred_element_type=jnp.float32)
    mixed_grad = jnp.dot(middle_b, w_out.T, preferred_element_type=jnp.float32).astype(jnp.bfloat16)
    mixed_grad = mixed_grad.reshape(IMG_GROUP, TILE, HEADS, HEAD_DIM).astype(jnp.float32)
    prob_grad = jnp.einsum('gqhd,gkhd->ghqk', mixed_grad, values_part)
    score_grad = probability * (prob_grad - lax.optimization_barrier(jnp.sum(probability * prob_grad, axis=-1, keepdims=True))) * scaling
    score_grad = score_grad.astype(jnp.bfloat16).astype(jnp.float32)
    q_grad = jnp.einsum('ghqk,gkhd->gqhd', score_grad, keys_part)
    k_grad = jnp.einsum('ghqk,gqhd->gkhd', score_grad, queries)
    v_grad = jnp.einsum('ghqk,gqhd->gkhd', prob_low.astype(jnp.float32), mixed_grad)
    packed_grad = jnp.stack([q_grad, k_grad, v_grad], axis=3).astype(jnp.bfloat16)
    packed_grad = packed_grad.reshape(rows_here, HEADS * 3 * HEAD_DIM)
    qkv_term = jnp.dot(normed_in.T, packed_grad, preferred_element_type=jnp.float32).reshape(D_VIT, HEADS, 3 * HEAD_DIM)
    heads_rank = HEADS // N_TP
    attn_parts = jnp.einsum('rtj,ctj->trc', packed_grad.reshape(rows_here, N_TP, heads_rank * 3 * HEAD_DIM).astype(jnp.float32), w_qkv.reshape(D_VIT, N_TP, heads_rank * 3 * HEAD_DIM).astype(jnp.float32))
    in_sum = lax.optimization_barrier(jnp.sum(chop(attn_parts), axis=0))
    in_back, ln1_term = norm_back(in_sum, normed1, inverse1, ln1_gain)
    grad_block = (upstream_f + in_back).astype(jnp.bfloat16)
    return ((qkv_term, out_term, ln1_term), grad_block)

def reference(grad_rows, features, block_in, patch_counts, owner, ln1_gain, w_qkv, w_out, w_proj):
    items = N_ENC * IMG_GROUP
    counts = patch_counts.reshape(-1).astype(jnp.int32)
    peers = jnp.arange(N_ENC, dtype=jnp.int32)
    sends = jnp.any(owner[:, :, None] == peers[None, None, :], axis=1).astype(jnp.int32)
    rank = (jnp.cumsum(sends, axis=0) - sends).astype(jnp.int32)
    own_rank = jnp.take_along_axis(rank, owner.astype(jnp.int32), axis=1)
    dest = (owner * IMG_GROUP + own_rank).reshape(-1).astype(jnp.int32)
    line = jnp.arange(TILE, dtype=jnp.int32)
    live_src = line[None, :] < counts[:, None]
    block_llm = D_LLM // N_TP
    vis_grad = jnp.zeros((N_ENC * ROWS_DEV, D_VIT), jnp.float32)
    for tp_block in range(N_TP):
        partial_value = jnp.dot(grad_rows[:, tp_block * block_llm:(tp_block + 1) * block_llm], w_proj[:, tp_block * block_llm:(tp_block + 1) * block_llm].T, preferred_element_type=jnp.float32)
        vis_grad = vis_grad + chop(partial_value)
    vis_tiles = jnp.where(live_src[:, :, None], vis_grad.reshape(items, TILE, D_VIT), jnp.zeros((), jnp.float32))
    upstream = jnp.zeros((items, TILE, D_VIT), jnp.float32).at[dest].set(vis_tiles).reshape(N_ENC * ROWS_DEV, D_VIT)
    dest_counts = jnp.zeros((items,), jnp.int32).at[dest].set(counts)
    live_dest = (line[None, :] < dest_counts[:, None]).reshape(N_ENC, IMG_GROUP, TILE)
    kept_rows = jnp.where(live_src.reshape(-1)[:, None], features, jnp.zeros_like(features))

    def add_projector(running, pair_rows):
        return (running + chop(jnp.dot(pair_rows[0].T, pair_rows[1], preferred_element_type=jnp.float32)), None)
    grad_proj = lax.scan(add_projector, jnp.zeros((D_VIT, D_LLM), jnp.float32), (kept_rows.reshape(N_ENC, ROWS_DEV, D_VIT), grad_rows.reshape(N_ENC, ROWS_DEV, D_LLM)))[0]

    def add_term(running_sum, new_term):
        return running_sum + chop(new_term)

    def one_block(running, pieces):
        terms, grad_block = block_backward(pieces[0], pieces[1], pieces[2], ln1_gain, w_qkv, w_out)
        return (jax.tree.map(add_term, running, terms), grad_block)
    start_sums = (jnp.zeros((D_VIT, HEADS, 3 * HEAD_DIM), jnp.float32), jnp.zeros((D_VIT, D_VIT), jnp.float32), jnp.zeros((D_VIT,), jnp.float32))
    sums_out, grad_blocks = lax.scan(one_block, start_sums, (block_in.reshape(N_ENC, ROWS_DEV, D_VIT), upstream.reshape(N_ENC, ROWS_DEV, D_VIT), live_dest))
    grad_input = grad_blocks.reshape(N_ENC * ROWS_DEV, D_VIT)
    return (grad_input, grad_proj, sums_out[0], sums_out[1], sums_out[2])
```

```python
import jax
import jax.numpy as jnp
from jax import lax
from jax.sharding import PartitionSpec as P

TILE = 128


EPSILON = 1e-05


def normalize(values):
    centred = values - jnp.mean(values, axis=-1, keepdims=True)
    variance = jnp.mean(centred * centred, axis=-1, keepdims=True)
    inverse = lax.rsqrt(variance + EPSILON)
    return (centred * inverse, inverse)


def dot_nt(left, right):
    return lax.dot_general(
        left, right, (((1,), (1,)), ((), ())), preferred_element_type=jnp.float32
    )


def dot_tn(left, right):
    return lax.dot_general(
        left, right, (((0,), (0,)), ((), ())), preferred_element_type=jnp.float32
    )


def inner_size(groups):
    inner = 1
    while inner * inner * 4 <= groups:
        inner *= 2
    return inner


def two_stage_sum(part, axis, inner):
    total = part.shape[0]
    outer = total // inner
    index = lax.axis_index(axis)
    at_outer, at_inner = index // inner, index % inner
    parts = part.reshape((outer, inner) + part.shape[1:])

    def pick(values, place, dim):
        return lax.dynamic_index_in_dim(values, place, dim, keepdims=False)

    running = pick(parts, at_inner, 1).astype(jnp.float32)
    for step in range(1, inner):
        pairs = [(o * inner + i, o * inner + (i + step) % inner) for o in range(outer) for i in range(inner)]
        running += lax.ppermute(pick(parts, (at_inner + step) % inner, 1), axis, pairs).astype(jnp.float32)
    summed = pick(running, at_outer, 0)
    short = running.astype(jnp.bfloat16)
    for step in range(1, outer):
        pairs = [(o * inner + i, (o + step) % outer * inner + i) for o in range(outer) for i in range(inner)]
        summed += lax.ppermute(pick(short, (at_outer + step) % outer, 0), axis, pairs).astype(jnp.float32)
    return summed


def summed_rows(part, axis, inner, cuts):
    rows = part.shape[1]
    if rows % (16 * cuts):
        cuts = 1
    height = rows // cuts
    pieces = [two_stage_sum(part[:, c * height : (c + 1) * height], axis, inner) for c in range(cuts)]
    return jnp.concatenate(pieces, axis=0) if cuts > 1 else pieces[0]


def gathered(share, axis):
    total = lax.axis_size(axis)
    index = lax.axis_index(axis)
    whole = jnp.zeros((total,) + share.shape, share.dtype)
    whole = lax.dynamic_update_index_in_dim(whole, share, index, 0)
    for step in range(1, total):
        pairs = [(i, (i + step) % total) for i in range(total)]
        whole = lax.dynamic_update_index_in_dim(
            whole, lax.ppermute(share, axis, pairs), (index - step) % total, 0
        )
    return whole


def shards(grad_rows, features, block_in, patch_counts, owner, ln1_gain, w_qkv, w_out, w_proj):
    groups = lax.axis_size("enc")
    tp_size = lax.axis_size("tp")
    inner = inner_size(groups)
    device = lax.axis_index("enc")
    tp_rank = lax.axis_index("tp")
    block_rows = grad_rows.shape[0]
    img_group = block_rows // TILE
    share_width = block_in.shape[1]
    features_dim = features.shape[1]
    line_index = jnp.arange(TILE, dtype=jnp.int32)
    peer_index = jnp.arange(groups, dtype=jnp.int32)
    own_counts = lax.dynamic_index_in_dim(patch_counts, device, 0, keepdims=False)
    own_owner = lax.dynamic_index_in_dim(owner, device, 0, keepdims=False)
    live_own = line_index[None, :] < own_counts[:, None]

    sends = jnp.any(owner == device, axis=1)
    sends_int = sends.astype(jnp.int32)
    rank = jnp.cumsum(sends_int) - sends_int
    slot_index = jnp.arange(img_group, dtype=jnp.int32)
    source_of = jnp.sum(
        jnp.where(sends[None, :] & (rank[None, :] == slot_index[:, None]), peer_index[None, :], 0),
        axis=1,
    )
    source_owner = jnp.take(owner, source_of, axis=0)
    source_counts = jnp.take(patch_counts, source_of, axis=0)
    arrived_counts = jnp.sum(jnp.where(source_owner == device, source_counts, 0), axis=1)
    live_tiles = line_index[None, :] < arrived_counts[:, None]

    vis_part = dot_nt(w_proj, grad_rows).astype(jnp.bfloat16)
    shared = two_stage_sum(vis_part.reshape(tp_size, share_width, block_rows), "tp", 2)
    tiles = jnp.where(live_own.reshape(-1)[None, :], shared, 0.0).astype(jnp.bfloat16)
    tiles = [tiles[:, j * TILE : (j + 1) * TILE] for j in range(img_group)]
    outgoing = jnp.zeros((groups, share_width, TILE), jnp.bfloat16)
    for j in range(img_group):
        outgoing = jnp.where((own_owner[j] == peer_index)[:, None, None], tiles[j][None], outgoing)
    received = lax.all_to_all(outgoing, "enc", split_axis=0, concat_axis=0, tiled=True)
    vis_share = jnp.concatenate(
        [lax.dynamic_index_in_dim(received, source_of[j], 0, keepdims=False) for j in range(img_group)],
        axis=1,
    )
    vis_low = gathered(vis_share, "tp").reshape(features_dim, block_rows)

    kept_rows = jnp.where(live_own.reshape(-1)[:, None], features, jnp.zeros_like(features))
    proj_term = dot_tn(kept_rows, grad_rows).astype(jnp.bfloat16)
    grad_proj = summed_rows(
        proj_term.reshape(groups, features_dim // groups, proj_term.shape[1]), "enc", inner, 2
    )

    heads_here = w_qkv.shape[1]
    head_size = w_qkv.shape[2] // 3
    block_full = gathered(block_in, "tp")
    block_full = jnp.concatenate([block_full[t] for t in range(tp_size)], axis=1)
    qkv_flat = w_qkv.reshape(features_dim, heads_here * 3 * head_size)
    normed1, inverse1 = normalize(block_full.astype(jnp.float32))
    normed_in = (normed1 * ln1_gain).astype(jnp.bfloat16)
    packed = jnp.dot(normed_in, qkv_flat, preferred_element_type=jnp.float32).astype(jnp.bfloat16)
    packed = packed.reshape(img_group, TILE, heads_here, 3, head_size)
    queries = packed[:, :, :, 0, :]
    keys_part = packed[:, :, :, 1, :]
    values_part = packed[:, :, :, 2, :]
    scaling = 1.0 / head_size**0.5
    scores = (
        jnp.einsum("gqhd,gkhd->ghqk", queries, keys_part, preferred_element_type=jnp.float32)
        * scaling
    )
    same_kind = (live_tiles[:, :, None] == live_tiles[:, None, :])[:, None]
    scores = jnp.where(same_kind, scores, -1e30)
    row_max = jnp.max(scores, axis=-1, keepdims=True)
    exp_terms = jnp.exp(scores - row_max)
    probability = exp_terms / jnp.sum(exp_terms, axis=-1, keepdims=True)
    prob_low = probability.astype(jnp.bfloat16)
    mixed = jnp.einsum(
        "ghqk,gkhd->gqhd", prob_low, values_part, preferred_element_type=jnp.float32
    ).astype(jnp.bfloat16)
    mixed = mixed.reshape(block_rows, heads_here * head_size)
    out_term = jnp.dot(vis_low, mixed, preferred_element_type=jnp.float32).astype(jnp.bfloat16)
    mixed_grad = lax.dot_general(
        vis_low, w_out, (((0,), (1,)), ((), ())), preferred_element_type=jnp.float32
    )
    mixed_grad = mixed_grad.astype(jnp.bfloat16).reshape(img_group, TILE, heads_here, head_size)
    prob_grad = jnp.einsum(
        "gqhd,gkhd->ghqk", mixed_grad, values_part, preferred_element_type=jnp.float32
    )
    score_grad = (
        probability
        * (prob_grad - jnp.sum(probability * prob_grad, axis=-1, keepdims=True))
        * scaling
    )
    score_grad = score_grad.astype(jnp.bfloat16)
    q_grad = jnp.einsum(
        "ghqk,gkhd->gqhd", score_grad, keys_part, preferred_element_type=jnp.float32
    )
    k_grad = jnp.einsum("ghqk,gqhd->gkhd", score_grad, queries, preferred_element_type=jnp.float32)
    v_grad = jnp.einsum("ghqk,gqhd->gkhd", prob_low, mixed_grad, preferred_element_type=jnp.float32)
    packed_grad = jnp.stack([q_grad, k_grad, v_grad], axis=3).astype(jnp.bfloat16)
    packed_grad = packed_grad.reshape(block_rows, heads_here * 3 * head_size)
    qkv_term = dot_tn(normed_in, packed_grad).astype(jnp.bfloat16)
    in_part = dot_nt(qkv_flat, packed_grad).astype(jnp.bfloat16)

    in_sum = two_stage_sum(in_part.reshape(tp_size, share_width, block_rows), "tp", 2).T
    centre = jnp.mean(block_full.astype(jnp.float32), axis=-1, keepdims=True)
    normed_share = (block_in.astype(jnp.float32) - centre) * inverse1
    gain_share = lax.dynamic_slice_in_dim(ln1_gain, tp_rank * share_width, share_width, 0)
    scaled = in_sum * gain_share
    sums = jnp.stack([jnp.sum(scaled, axis=-1), jnp.sum(scaled * normed_share, axis=-1)])
    ln1_share = jnp.sum(in_sum * normed_share, axis=0)
    small = jnp.concatenate([sums.reshape(-1), ln1_share])
    small = gathered(small, "tp")
    means = jnp.sum(small[:, : 2 * block_rows], axis=0).reshape(2, block_rows, 1) / features_dim
    in_back = inverse1 * (scaled - means[0] - normed_share * means[1])
    vis_own = vis_share.astype(jnp.float32).T
    grad_input = (vis_own + in_back).astype(jnp.bfloat16)

    ln1_term = small[:, 2 * block_rows :].reshape(groups, features_dim // groups).astype(jnp.bfloat16)
    grad_qkv = summed_rows(
        qkv_term.reshape(groups, features_dim // groups, qkv_term.shape[1]), "enc", inner, 2
    ).reshape(features_dim // groups, heads_here, 3 * head_size)
    grad_out = two_stage_sum(
        out_term.reshape(groups, features_dim // groups, out_term.shape[1]), "enc", inner
    ).T
    grad_ln1 = two_stage_sum(ln1_term, "enc", inner)
    return (grad_input, grad_proj, grad_qkv, grad_out, grad_ln1)


def solution(mesh):
    placed = (
        P("enc", "tp"),
        P("enc", None),
        P("enc", "tp"),
        P(),
        P(),
        P(),
        P(None, "tp", None),
        P("tp", None),
        P(None, "tp"),
    )
    return jax.shard_map(
        shards,
        mesh=mesh,
        in_specs=placed,
        out_specs=(P("enc", "tp"), P("enc", "tp"), P("enc", "tp", None), P("tp", "enc"), P("enc")),
        check_vma=False,
    )
```

```python
import jax
import jax.numpy as jnp
from jax import lax
from jax.experimental import pallas as pl
from jax.experimental.pallas import tpu as pltpu
from jax.sharding import PartitionSpec as P

TILE = 128


EPSILON = 1e-05


def normalize(values):
    centred = values - jnp.mean(values, axis=-1, keepdims=True)
    variance = jnp.mean(centred * centred, axis=-1, keepdims=True)
    inverse = lax.rsqrt(variance + EPSILON)
    return (centred * inverse, inverse)


def dot_nt(left, right):
    return lax.dot_general(
        left, right, (((1,), (1,)), ((), ())), preferred_element_type=jnp.float32
    )


def dot_tn(left, right):
    return lax.dot_general(
        left, right, (((0,), (0,)), ((), ())), preferred_element_type=jnp.float32
    )


def inner_size(groups):
    inner = 1
    while inner * inner * 4 <= groups:
        inner *= 2
    return inner


def pick(values, place, dim):
    return lax.dynamic_index_in_dim(values, place, dim, keepdims=False, allow_negative_indices=False)


def two_stage_sum(left, right, axis, inner, name):
    total = left.shape[0]
    outer = total // inner
    index = lax.axis_index(axis).astype(jnp.uint32)
    at_outer, at_inner = lax.div(index, jnp.uint32(inner)), lax.rem(index, jnp.uint32(inner))
    lefts = left.reshape((outer, inner) + left.shape[1:])

    def term(place):
        chosen = pick(lefts, place, 1)
        flat = chosen.reshape(-1, chosen.shape[-1])
        product = jnp.dot(flat, right, preferred_element_type=jnp.float32).astype(jnp.bfloat16)
        return product.reshape(outer, -1, right.shape[1])

    arrived = []
    for step in range(1, inner):
        pairs = [(o * inner + i, o * inner + (i + step) % inner) for o in range(outer) for i in range(inner)]
        sent = term(lax.rem(at_inner + jnp.uint32(step), jnp.uint32(inner)))
        with jax.named_scope(name + "_first"):
            arrived.append(lax.ppermute(sent, axis, pairs))
    running = term(at_inner).astype(jnp.float32)
    with jax.named_scope(name + "_add"):
        for value in arrived:
            running += value.astype(jnp.float32)
        summed = pick(running, at_outer, 0)
        short = running.astype(jnp.bfloat16)
    arrived = []
    for step in range(1, outer):
        pairs = [(o * inner + i, (o + step) % outer * inner + i) for o in range(outer) for i in range(inner)]
        sent = pick(short, lax.rem(at_outer + jnp.uint32(step), jnp.uint32(outer)), 0)
        with jax.named_scope(name + "_second"):
            arrived.append(lax.ppermute(sent, axis, pairs))
    with jax.named_scope(name + "_end"):
        for value in arrived:
            summed += value.astype(jnp.float32)
    return summed


def summed_rows(left, right, axis, inner, cuts, name):
    rows = left.shape[1]
    if rows % (16 * cuts):
        cuts = 1
    height = rows // cuts
    pieces = [
        two_stage_sum(left[:, c * height : (c + 1) * height], right, axis, inner, name + str(c))
        for c in range(cuts)
    ]
    return jnp.concatenate(pieces, axis=0) if cuts > 1 else pieces[0]


def small_sum(part, axis):
    total = part.shape[0]
    index = lax.axis_index(axis).astype(jnp.uint32)
    summed = pick(part, index, 0).astype(jnp.float32)
    for step in range(1, total):
        pairs = [(i, (i + step) % total) for i in range(total)]
        sent = pick(part, lax.rem(index + jnp.uint32(step), jnp.uint32(total)), 0)
        with jax.named_scope("ln1"):
            summed += lax.ppermute(sent, axis, pairs).astype(jnp.float32)
    return summed


def attend_kernel(size, counts_ref, packed_ref, prob_ref, mixed_ref):
    tile = packed_ref.shape[0]
    count = counts_ref[pl.program_id(0)]
    rows = lax.broadcasted_iota(jnp.int32, (tile, tile), 0) < count
    columns = lax.broadcasted_iota(jnp.int32, (tile, tile), 1) < count
    same = jnp.logical_not(jnp.logical_xor(rows, columns))
    scaling = 1.0 / size**0.5
    for h in range(prob_ref.shape[1]):
        base = h * 3 * size
        queries = packed_ref[:, base : base + size]
        keys = packed_ref[:, base + size : base + 2 * size]
        values = packed_ref[:, base + 2 * size : base + 3 * size]
        scores = jnp.where(same, dot_nt(queries, keys) * scaling, -1e30)
        terms = jnp.exp(scores - jnp.max(scores, axis=-1, keepdims=True))
        probability = terms / jnp.sum(terms, axis=-1, keepdims=True)
        prob_ref[0, h] = probability
        mixed = jnp.dot(probability.astype(jnp.bfloat16), values, preferred_element_type=jnp.float32)
        mixed_ref[:, h * size : (h + 1) * size] = mixed.astype(jnp.bfloat16)


def attend(packed, counts, heads, size):
    rows = packed.shape[0]
    images = rows // TILE
    return pl.pallas_call(
        lambda *refs: attend_kernel(size, *refs),
        grid=(images,),
        in_specs=[
            pl.BlockSpec(memory_space=pltpu.SMEM),
            pl.BlockSpec((TILE, packed.shape[1]), lambda i: (i, 0)),
        ],
        out_specs=[
            pl.BlockSpec((1, heads, TILE, TILE), lambda i: (i, 0, 0, 0)),
            pl.BlockSpec((TILE, heads * size), lambda i: (i, 0)),
        ],
        out_shape=[
            jax.ShapeDtypeStruct((images, heads, TILE, TILE), jnp.float32),
            jax.ShapeDtypeStruct((rows, heads * size), jnp.bfloat16),
        ],
        cost_estimate=pl.CostEstimate(flops=2 * 10**9, bytes_accessed=4 * 10**6, transcendentals=0),
        name="attend",
    )(counts, packed)


def attend_back_kernel(size, packed_ref, prob_ref, vis_ref, out_ref, grad_ref):
    scaling = 1.0 / size**0.5
    mixed_grads = lax.dot_general(
        vis_ref[...], out_ref[...], (((0,), (1,)), ((), ())), preferred_element_type=jnp.float32
    ).astype(jnp.bfloat16)
    for h in range(prob_ref.shape[1]):
        base = h * 3 * size
        queries = packed_ref[:, base : base + size]
        keys = packed_ref[:, base + size : base + 2 * size]
        values = packed_ref[:, base + 2 * size : base + 3 * size]
        mixed_grad = mixed_grads[:, h * size : (h + 1) * size]
        probability = prob_ref[0, h]
        prob_grad = dot_nt(mixed_grad, values)
        inner = jnp.sum(probability * prob_grad, axis=-1, keepdims=True)
        score_grad = (probability * (prob_grad - inner) * scaling).astype(jnp.bfloat16)
        prob_low = probability.astype(jnp.bfloat16)
        q_grad = jnp.dot(score_grad, keys, preferred_element_type=jnp.float32)
        grad_ref[:, base : base + size] = q_grad.astype(jnp.bfloat16)
        grad_ref[:, base + size : base + 2 * size] = dot_tn(score_grad, queries).astype(jnp.bfloat16)
        grad_ref[:, base + 2 * size : base + 3 * size] = dot_tn(prob_low, mixed_grad).astype(jnp.bfloat16)


def attend_back(packed, probability, vis_low, w_out, size):
    rows, width = packed.shape
    images, heads = probability.shape[:2]
    return pl.pallas_call(
        lambda *refs: attend_back_kernel(size, *refs),
        grid=(images,),
        in_specs=[
            pl.BlockSpec((TILE, width), lambda i: (i, 0)),
            pl.BlockSpec((1, heads, TILE, TILE), lambda i: (i, 0, 0, 0)),
            pl.BlockSpec((vis_low.shape[0], TILE), lambda i: (0, i)),
            pl.BlockSpec(w_out.shape, lambda i: (0, 0)),
        ],
        out_specs=pl.BlockSpec((TILE, width), lambda i: (i, 0)),
        out_shape=jax.ShapeDtypeStruct((rows, width), jnp.bfloat16),
        cost_estimate=pl.CostEstimate(flops=3 * 10**9, bytes_accessed=6 * 10**6, transcendentals=0),
        name="attend_back",
    )(packed, probability, vis_low, w_out)


def gathered(share, axis, name):
    total = lax.axis_size(axis)
    index = lax.axis_index(axis).astype(jnp.uint32)
    stacked = [share]
    for step in range(1, total):
        pairs = [(i, (i - step) % total) for i in range(total)]
        with jax.named_scope(name):
            stacked.append(lax.ppermute(share, axis, pairs))
    twice = jnp.concatenate([part[None] for part in stacked + stacked[:-1]], axis=0)
    return lax.dynamic_slice_in_dim(twice, lax.rem(jnp.uint32(total) - index, jnp.uint32(total)), total, 0) if total > 1 else twice


def shards(grad_rows, features, block_in, patch_counts, owner, ln1_gain, w_qkv, w_out, w_proj):
    groups = lax.axis_size("enc")
    tp_size = lax.axis_size("tp")
    inner = inner_size(groups)
    device = lax.axis_index("enc")
    tp_rank = lax.axis_index("tp")
    block_rows = grad_rows.shape[0]
    img_group = block_rows // TILE
    share_width = block_in.shape[1]
    features_dim = features.shape[1]
    line_index = jnp.arange(TILE, dtype=jnp.int32)
    peer_index = jnp.arange(groups, dtype=jnp.int32)
    own_counts = lax.dynamic_index_in_dim(patch_counts, device, 0, keepdims=False)
    own_owner = lax.dynamic_index_in_dim(owner, device, 0, keepdims=False)
    live_own = line_index[None, :] < own_counts[:, None]

    sends = jnp.any(owner == device, axis=1)
    sends_int = sends.astype(jnp.int32)
    rank = jnp.cumsum(sends_int) - sends_int
    slot_index = jnp.arange(img_group, dtype=jnp.int32)
    source_of = jnp.sum(
        jnp.where(sends[None, :] & (rank[None, :] == slot_index[:, None]), peer_index[None, :], 0),
        axis=1,
    )
    source_owner = jnp.take(owner, source_of, axis=0)
    source_counts = jnp.take(patch_counts, source_of, axis=0)
    arrived_counts = jnp.sum(jnp.where(source_owner == device, source_counts, 0), axis=1)
    live_tiles = line_index[None, :] < arrived_counts[:, None]

    kept_rows = jnp.where(live_own.reshape(-1)[:, None], features, jnp.zeros_like(features))
    piece_rows = features_dim // groups
    grad_proj = summed_rows(
        kept_rows.T.reshape(groups, piece_rows, block_rows), grad_rows, "enc", inner, 2, "proj"
    )

    shared = two_stage_sum(
        w_proj.reshape(tp_size, share_width, w_proj.shape[1]), grad_rows.T, "tp", 2, "vis"
    )
    tiles = jnp.where(live_own.reshape(-1)[None, :], shared, 0.0).astype(jnp.bfloat16)
    tiles = [tiles[:, j * TILE : (j + 1) * TILE] for j in range(img_group)]
    outgoing = jnp.zeros((groups, share_width, TILE), jnp.bfloat16)
    for j in range(img_group):
        outgoing = jnp.where((own_owner[j] == peer_index)[:, None, None], tiles[j][None], outgoing)
    with jax.named_scope("route"):
        received = lax.all_to_all(outgoing, "enc", split_axis=0, concat_axis=0, tiled=True)
    vis_share = jnp.concatenate(
        [lax.dynamic_index_in_dim(received, source_of[j], 0, keepdims=False) for j in range(img_group)],
        axis=1,
    )
    vis_low = gathered(vis_share, "tp", "visall").reshape(features_dim, block_rows)

    heads_here = w_qkv.shape[1]
    head_size = w_qkv.shape[2] // 3
    block_full = gathered(block_in, "tp", "blockall")
    block_full = jnp.concatenate([block_full[t] for t in range(tp_size)], axis=1)
    qkv_flat = w_qkv.reshape(features_dim, heads_here * 3 * head_size)
    normed1, inverse1 = normalize(block_full.astype(jnp.float32))
    normed_in = (normed1 * ln1_gain).astype(jnp.bfloat16)
    packed = jnp.dot(normed_in, qkv_flat, preferred_element_type=jnp.float32).astype(jnp.bfloat16)
    probability, mixed = attend(packed, arrived_counts, heads_here, head_size)
    packed_grad = attend_back(packed, probability, vis_low, w_out, head_size)

    in_sum = two_stage_sum(
        qkv_flat.reshape(tp_size, share_width, qkv_flat.shape[1]), packed_grad.T, "tp", 2, "insum"
    ).T
    centre = jnp.mean(block_full.astype(jnp.float32), axis=-1, keepdims=True)
    normed_share = (block_in.astype(jnp.float32) - centre) * inverse1
    gain_share = lax.dynamic_slice_in_dim(ln1_gain, tp_rank * share_width, share_width, 0)
    scaled = in_sum * gain_share
    sums = jnp.stack([jnp.sum(scaled, axis=-1), jnp.sum(scaled * normed_share, axis=-1)])
    ln1_share = jnp.sum(in_sum * normed_share, axis=0)
    small = jnp.concatenate([sums.reshape(-1), ln1_share])
    small = gathered(small, "tp", "smallall")
    means = jnp.sum(small[:, : 2 * block_rows], axis=0).reshape(2, block_rows, 1) / features_dim
    in_back = inverse1 * (scaled - means[0] - normed_share * means[1])
    vis_own = vis_share.astype(jnp.float32).T
    grad_input = (vis_own + in_back).astype(jnp.bfloat16)

    grad_qkv = summed_rows(
        normed_in.T.reshape(groups, piece_rows, block_rows), packed_grad, "enc", inner, 2, "qkv"
    ).reshape(piece_rows, heads_here, 3 * head_size)
    grad_out = two_stage_sum(
        vis_low.reshape(groups, piece_rows, block_rows), mixed, "enc", inner, "out"
    ).T
    ln1_term = small[:, 2 * block_rows :].reshape(groups, piece_rows).astype(jnp.bfloat16)
    grad_ln1 = small_sum(ln1_term, "enc")
    return (grad_input, grad_proj, grad_qkv, grad_out, grad_ln1)


def solution(mesh):
    placed = (
        P("enc", "tp"),
        P("enc", None),
        P("enc", "tp"),
        P(),
        P(),
        P(),
        P(None, "tp", None),
        P("tp", None),
        P(None, "tp"),
    )
    return jax.shard_map(
        shards,
        mesh=mesh,
        in_specs=placed,
        out_specs=(P("enc", "tp"), P("enc", "tp"), P("enc", "tp", None), P("tp", "enc"), P("enc")),
        check_vma=False,
    )
```

```python
import jax
import jax.numpy as jnp
from jax import lax
from jax.experimental import pallas as pl
from jax.experimental.pallas import tpu as pltpu
from jax.sharding import PartitionSpec as P


TILE = 128


EPSILON = 1e-05


def dot_nt(left, right):
    return lax.dot_general(
        left, right, (((1,), (1,)), ((), ())), preferred_element_type=jnp.float32
    )


def dot_tn(left, right):
    return lax.dot_general(
        left, right, (((0,), (0,)), ((), ())), preferred_element_type=jnp.float32
    )


def inner_size(groups):
    inner = 1
    while inner * inner * 4 <= groups:
        inner *= 2
    return inner


def pick(values, place, dim):
    return lax.dynamic_index_in_dim(values, place, dim, keepdims=False, allow_negative_indices=False)


def two_stage_sum(left, right, axis, inner, whole=False):
    total = left.shape[0]
    outer = total // inner
    index = lax.axis_index(axis).astype(jnp.uint32)
    at_outer, at_inner = lax.div(index, jnp.uint32(inner)), lax.rem(index, jnp.uint32(inner))
    lefts = left.reshape((outer, inner) + left.shape[1:])

    if whole:
        every = jnp.dot(left.reshape(-1, left.shape[2]), right, preferred_element_type=jnp.float32)
        every = every.astype(jnp.bfloat16).reshape((outer, inner) + (left.shape[1], right.shape[1]))

    def term(place):
        if whole:
            return pick(every, place, 1)
        chosen = pick(lefts, place, 1)
        flat = chosen.reshape(-1, chosen.shape[-1])
        product = jnp.dot(flat, right, preferred_element_type=jnp.float32).astype(jnp.bfloat16)
        return product.reshape(outer, -1, right.shape[1])

    arrived = []
    for step in range(1, inner):
        pairs = [(o * inner + i, o * inner + (i + step) % inner) for o in range(outer) for i in range(inner)]
        sent = term(lax.rem(at_inner + jnp.uint32(step), jnp.uint32(inner)))
        arrived.append(lax.ppermute(sent, axis, pairs))
    running = term(at_inner).astype(jnp.float32)
    for value in arrived:
        running += value.astype(jnp.float32)
    summed = pick(running, at_outer, 0)
    short = running.astype(jnp.bfloat16)
    arrived = []
    for step in range(1, outer):
        pairs = [(o * inner + i, (o + step) % outer * inner + i) for o in range(outer) for i in range(inner)]
        sent = pick(short, lax.rem(at_outer + jnp.uint32(step), jnp.uint32(outer)), 0)
        arrived.append(lax.ppermute(sent, axis, pairs))
    for value in arrived:
        summed += value.astype(jnp.float32)
    return summed


def summed_rows(left, right, axis, inner, cuts):
    rows = left.shape[1]
    if rows % (16 * cuts):
        cuts = 1
    height = rows // cuts
    pieces = [two_stage_sum(left[:, c * height : (c + 1) * height], right, axis, inner) for c in range(cuts)]
    return jnp.concatenate(pieces, axis=0) if cuts > 1 else pieces[0]


def small_sum(part, axis):
    total = part.shape[0]
    index = lax.axis_index(axis).astype(jnp.uint32)
    summed = pick(part, index, 0).astype(jnp.float32)
    for step in range(1, total):
        pairs = [(i, (i + step) % total) for i in range(total)]
        sent = pick(part, lax.rem(index + jnp.uint32(step), jnp.uint32(total)), 0)
        summed += lax.ppermute(sent, axis, pairs).astype(jnp.float32)
    return summed


def attend_kernel(size, counts_ref, packed_ref, prob_ref, mixed_ref):
    tile = packed_ref.shape[0]
    count = counts_ref[pl.program_id(0)]
    rows = lax.broadcasted_iota(jnp.int32, (tile, tile), 0) < count
    columns = lax.broadcasted_iota(jnp.int32, (tile, tile), 1) < count
    same = jnp.logical_not(jnp.logical_xor(rows, columns))
    scaling = 1.0 / size**0.5
    for h in range(prob_ref.shape[1]):
        base = h * 3 * size
        queries = packed_ref[:, base : base + size]
        keys = packed_ref[:, base + size : base + 2 * size]
        values = packed_ref[:, base + 2 * size : base + 3 * size]
        scores = jnp.where(same, dot_nt(queries, keys) * scaling, -1e30)
        terms = jnp.exp(scores - jnp.max(scores, axis=-1, keepdims=True))
        probability = terms / jnp.sum(terms, axis=-1, keepdims=True)
        prob_ref[0, h] = probability
        mixed = jnp.dot(probability.astype(jnp.bfloat16), values, preferred_element_type=jnp.float32)
        mixed_ref[:, h * size : (h + 1) * size] = mixed.astype(jnp.bfloat16)


def attend(packed, counts, heads, size):
    rows = packed.shape[0]
    images = rows // TILE
    return pl.pallas_call(
        lambda *refs: attend_kernel(size, *refs),
        grid=(images,),
        in_specs=[
            pl.BlockSpec(memory_space=pltpu.SMEM),
            pl.BlockSpec((TILE, packed.shape[1]), lambda i: (i, 0)),
        ],
        out_specs=[
            pl.BlockSpec((1, heads, TILE, TILE), lambda i: (i, 0, 0, 0)),
            pl.BlockSpec((TILE, heads * size), lambda i: (i, 0)),
        ],
        out_shape=[
            jax.ShapeDtypeStruct((images, heads, TILE, TILE), jnp.float32),
            jax.ShapeDtypeStruct((rows, heads * size), jnp.bfloat16),
        ],
        cost_estimate=pl.CostEstimate(flops=2 * 10**9, bytes_accessed=4 * 10**6, transcendentals=0),
        name="attend",
    )(counts, packed)


def attend_back_kernel(size, packed_ref, prob_ref, vis_ref, out_ref, grad_ref):
    scaling = 1.0 / size**0.5
    mixed_grads = lax.dot_general(
        vis_ref[...], out_ref[...], (((0,), (1,)), ((), ())), preferred_element_type=jnp.float32
    ).astype(jnp.bfloat16)
    for h in range(prob_ref.shape[1]):
        base = h * 3 * size
        queries = packed_ref[:, base : base + size]
        keys = packed_ref[:, base + size : base + 2 * size]
        values = packed_ref[:, base + 2 * size : base + 3 * size]
        mixed_grad = mixed_grads[:, h * size : (h + 1) * size]
        probability = prob_ref[0, h]
        prob_grad = dot_nt(mixed_grad, values)
        inner = jnp.sum(probability * prob_grad, axis=-1, keepdims=True)
        score_grad = (probability * (prob_grad - inner) * scaling).astype(jnp.bfloat16)
        prob_low = probability.astype(jnp.bfloat16)
        q_grad = jnp.dot(score_grad, keys, preferred_element_type=jnp.float32)
        grad_ref[:, base : base + size] = q_grad.astype(jnp.bfloat16)
        grad_ref[:, base + size : base + 2 * size] = dot_tn(score_grad, queries).astype(jnp.bfloat16)
        grad_ref[:, base + 2 * size : base + 3 * size] = dot_tn(prob_low, mixed_grad).astype(jnp.bfloat16)


def attend_back(packed, probability, vis_low, w_out, size):
    rows, width = packed.shape
    images, heads = probability.shape[:2]
    return pl.pallas_call(
        lambda *refs: attend_back_kernel(size, *refs),
        grid=(images,),
        in_specs=[
            pl.BlockSpec((TILE, width), lambda i: (i, 0)),
            pl.BlockSpec((1, heads, TILE, TILE), lambda i: (i, 0, 0, 0)),
            pl.BlockSpec((vis_low.shape[0], TILE), lambda i: (0, i)),
            pl.BlockSpec(w_out.shape, lambda i: (0, 0)),
        ],
        out_specs=pl.BlockSpec((TILE, width), lambda i: (i, 0)),
        out_shape=jax.ShapeDtypeStruct((rows, width), jnp.bfloat16),
        cost_estimate=pl.CostEstimate(flops=3 * 10**9, bytes_accessed=6 * 10**6, transcendentals=0),
        name="attend_back",
    )(packed, probability, vis_low, w_out)


def gathered(share, axis):
    total = lax.axis_size(axis)
    index = lax.axis_index(axis).astype(jnp.uint32)
    stacked = [share]
    for step in range(1, total):
        pairs = [(i, (i - step) % total) for i in range(total)]
        stacked.append(lax.ppermute(share, axis, pairs))
    twice = jnp.concatenate([part[None] for part in stacked + stacked[:-1]], axis=0)
    return lax.dynamic_slice_in_dim(twice, lax.rem(jnp.uint32(total) - index, jnp.uint32(total)), total, 0) if total > 1 else twice


def shards(grad_rows, features, block_in, patch_counts, owner, ln1_gain, w_qkv, w_out, w_proj):
    groups = lax.axis_size("enc")
    tp_size = lax.axis_size("tp")
    inner = inner_size(groups)
    device = lax.axis_index("enc")
    tp_rank = lax.axis_index("tp")
    block_rows = grad_rows.shape[0]
    img_group = block_rows // TILE
    share_width = block_in.shape[1]
    features_dim = features.shape[1]
    line_index = jnp.arange(TILE, dtype=jnp.int32)
    peer_index = jnp.arange(groups, dtype=jnp.int32)
    own_counts = lax.dynamic_index_in_dim(patch_counts, device, 0, keepdims=False)
    own_owner = lax.dynamic_index_in_dim(owner, device, 0, keepdims=False)
    live_own = line_index[None, :] < own_counts[:, None]

    sends = jnp.any(owner == device, axis=1)
    sends_int = sends.astype(jnp.int32)
    rank = jnp.cumsum(sends_int) - sends_int
    slot_index = jnp.arange(img_group, dtype=jnp.int32)
    source_of = jnp.sum(
        jnp.where(sends[None, :] & (rank[None, :] == slot_index[:, None]), peer_index[None, :], 0),
        axis=1,
    )
    source_owner = jnp.take(owner, source_of, axis=0)
    source_counts = jnp.take(patch_counts, source_of, axis=0)
    arrived_counts = jnp.sum(jnp.where(source_owner == device, source_counts, 0), axis=1)

    kept_rows = jnp.where(live_own.reshape(-1)[:, None], features, jnp.zeros_like(features))
    piece_rows = features_dim // groups
    grad_proj = summed_rows(kept_rows.T.reshape(groups, piece_rows, block_rows), grad_rows, "enc", inner, 2)

    shared = two_stage_sum(w_proj.reshape(tp_size, share_width, w_proj.shape[1]), grad_rows.T, "tp", 2, whole=True)
    tiles = jnp.where(live_own.reshape(-1)[None, :], shared, 0.0).astype(jnp.bfloat16)
    tiles = [tiles[:, j * TILE : (j + 1) * TILE] for j in range(img_group)]
    outgoing = jnp.zeros((groups, share_width, TILE), jnp.bfloat16)
    for j in range(img_group):
        outgoing = jnp.where((own_owner[j] == peer_index)[:, None, None], tiles[j][None], outgoing)
    received = lax.all_to_all(outgoing, "enc", split_axis=0, concat_axis=0, tiled=True)
    vis_share = jnp.concatenate([pick(received, source_of[j].astype(jnp.uint32), 0) for j in range(img_group)], axis=1)
    vis_low = gathered(vis_share, "tp").reshape(features_dim, block_rows)

    heads_here = w_qkv.shape[1]
    head_size = w_qkv.shape[2] // 3
    block_turned = block_in.T
    block_full = gathered(block_turned, "tp").reshape(features_dim, block_rows)
    qkv_flat = w_qkv.reshape(features_dim, heads_here * 3 * head_size)
    block_wide = block_full.astype(jnp.float32)
    centre = jnp.mean(block_wide, axis=0, keepdims=True)
    centred = block_wide - centre
    inverse1 = lax.rsqrt(jnp.mean(centred * centred, axis=0, keepdims=True) + EPSILON)
    normed_in = (centred * inverse1 * ln1_gain[:, None]).astype(jnp.bfloat16)
    packed = dot_tn(normed_in, qkv_flat).astype(jnp.bfloat16)
    probability, mixed = attend(packed, arrived_counts, heads_here, head_size)
    packed_grad = attend_back(packed, probability, vis_low, w_out, head_size)

    in_sum = two_stage_sum(
        qkv_flat.reshape(tp_size, share_width, qkv_flat.shape[1]), packed_grad.T, "tp", 2, whole=True
    )
    normed_share = (block_turned.astype(jnp.float32) - centre) * inverse1
    gain_share = lax.dynamic_slice_in_dim(ln1_gain, tp_rank * share_width, share_width, 0)
    scaled = in_sum * gain_share[:, None]
    sums = jnp.concatenate([jnp.sum(scaled, axis=0), jnp.sum(scaled * normed_share, axis=0)])
    ln1_share = jnp.sum(in_sum * normed_share, axis=1)
    small = jnp.concatenate([sums, ln1_share])
    small = gathered(small, "tp")
    means = jnp.sum(small[:, : 2 * block_rows], axis=0).reshape(2, 1, block_rows) / features_dim
    in_back = inverse1 * (scaled - means[0] - normed_share * means[1])
    grad_input = (vis_share.astype(jnp.float32) + in_back).astype(jnp.bfloat16).T

    grad_qkv = summed_rows(
        normed_in.reshape(groups, piece_rows, block_rows), packed_grad, "enc", inner, 2
    ).reshape(piece_rows, heads_here, 3 * head_size)
    grad_out = two_stage_sum(vis_low.reshape(groups, piece_rows, block_rows), mixed, "enc", inner).T
    ln1_term = small[:, 2 * block_rows :].reshape(groups, piece_rows).astype(jnp.bfloat16)
    grad_ln1 = small_sum(ln1_term, "enc")
    return (grad_input, grad_proj, grad_qkv, grad_out, grad_ln1)


def solution(mesh):
    placed = (
        P("enc", "tp"),
        P("enc", None),
        P("enc", "tp"),
        P(),
        P(),
        P(),
        P(None, "tp", None),
        P("tp", None),
        P(None, "tp"),
    )
    return jax.shard_map(
        shards,
        mesh=mesh,
        in_specs=placed,
        out_specs=(P("enc", "tp"), P("enc", "tp"), P("enc", "tp", None), P("tp", "enc"), P("enc")),
        check_vma=False,
    )
```

```python
import jax
import jax.numpy as jnp
from jax import lax
from jax.experimental import pallas as pl
from jax.experimental.pallas import tpu as pltpu
from jax.sharding import PartitionSpec as P


TILE = 128


EPSILON = 1e-05


def dot_nt(left, right):
    return lax.dot_general(
        left, right, (((1,), (1,)), ((), ())), preferred_element_type=jnp.float32
    )


def dot_tn(left, right):
    return lax.dot_general(
        left, right, (((0,), (0,)), ((), ())), preferred_element_type=jnp.float32
    )


def inner_size(groups):
    inner = 1
    while inner * inner * 4 <= groups:
        inner *= 2
    return inner


def pick(values, place, dim):
    return lax.dynamic_index_in_dim(values, place, dim, keepdims=False, allow_negative_indices=False)


def two_stage_sum(left, right, axis, inner):
    total = left.shape[0]
    outer = total // inner
    index = lax.axis_index(axis).astype(jnp.uint32)
    at_outer, at_inner = lax.div(index, jnp.uint32(inner)), lax.rem(index, jnp.uint32(inner))
    lefts = left.reshape((outer, inner) + left.shape[1:])

    def term(place):
        chosen = pick(lefts, place, 1)
        if right is None:
            return chosen
        flat = chosen.reshape(-1, chosen.shape[-1])
        product = jnp.dot(flat, right, preferred_element_type=jnp.float32).astype(jnp.bfloat16)
        return product.reshape(outer, -1, right.shape[1])

    arrived = []
    for step in range(1, inner):
        pairs = [(o * inner + i, o * inner + (i + step) % inner) for o in range(outer) for i in range(inner)]
        sent = term(lax.rem(at_inner + jnp.uint32(step), jnp.uint32(inner)))
        arrived.append(lax.ppermute(sent, axis, pairs))
    running = term(at_inner).astype(jnp.float32)
    for value in arrived:
        running += value.astype(jnp.float32)
    summed = pick(running, at_outer, 0)
    short = running.astype(jnp.bfloat16)
    arrived = []
    for step in range(1, outer):
        pairs = [(o * inner + i, (o + step) % outer * inner + i) for o in range(outer) for i in range(inner)]
        sent = pick(short, lax.rem(at_outer + jnp.uint32(step), jnp.uint32(outer)), 0)
        arrived.append(lax.ppermute(sent, axis, pairs))
    for value in arrived:
        summed += value.astype(jnp.float32)
    return summed


def summed_rows(left, right, axis, inner, cuts):
    rows = left.shape[1]
    if rows % (16 * cuts):
        cuts = 1
    height = rows // cuts
    pieces = [two_stage_sum(left[:, c * height : (c + 1) * height], right, axis, inner) for c in range(cuts)]
    return jnp.concatenate(pieces, axis=0) if cuts > 1 else pieces[0]


def attend_kernel(size, counts_ref, packed_ref, prob_ref, mixed_ref):
    tile = packed_ref.shape[0]
    count = counts_ref[pl.program_id(0)]
    rows = lax.broadcasted_iota(jnp.int32, (tile, tile), 0) < count
    columns = lax.broadcasted_iota(jnp.int32, (tile, tile), 1) < count
    same = jnp.logical_not(jnp.logical_xor(rows, columns))
    scaling = 1.0 / size**0.5
    for h in range(prob_ref.shape[1]):
        base = h * 3 * size
        queries = packed_ref[:, base : base + size]
        keys = packed_ref[:, base + size : base + 2 * size]
        values = packed_ref[:, base + 2 * size : base + 3 * size]
        scores = jnp.where(same, dot_nt(queries, keys) * scaling, -1e30)
        terms = jnp.exp(scores - jnp.max(scores, axis=-1, keepdims=True))
        probability = terms / jnp.sum(terms, axis=-1, keepdims=True)
        prob_ref[0, h] = probability
        mixed = jnp.dot(probability.astype(jnp.bfloat16), values, preferred_element_type=jnp.float32)
        mixed_ref[:, h * size : (h + 1) * size] = mixed.astype(jnp.bfloat16)


def attend(packed, counts, heads, size):
    rows = packed.shape[0]
    images = rows // TILE
    return pl.pallas_call(
        lambda *refs: attend_kernel(size, *refs),
        grid=(images,),
        in_specs=[
            pl.BlockSpec(memory_space=pltpu.SMEM),
            pl.BlockSpec((TILE, packed.shape[1]), lambda i: (i, 0)),
        ],
        out_specs=[
            pl.BlockSpec((1, heads, TILE, TILE), lambda i: (i, 0, 0, 0)),
            pl.BlockSpec((TILE, heads * size), lambda i: (i, 0)),
        ],
        out_shape=[
            jax.ShapeDtypeStruct((images, heads, TILE, TILE), jnp.float32),
            jax.ShapeDtypeStruct((rows, heads * size), jnp.bfloat16),
        ],
        cost_estimate=pl.CostEstimate(flops=2 * 10**9, bytes_accessed=4 * 10**6, transcendentals=0),
        name="attend",
    )(counts, packed)


def attend_back_kernel(size, packed_ref, prob_ref, vis_ref, out_ref, qkv_ref, grad_ref, part_ref):
    scaling = 1.0 / size**0.5
    mixed_grads = lax.dot_general(
        vis_ref[...], out_ref[...], (((0,), (1,)), ((), ())), preferred_element_type=jnp.float32
    ).astype(jnp.bfloat16)
    for h in range(prob_ref.shape[1]):
        base = h * 3 * size
        queries = packed_ref[:, base : base + size]
        keys = packed_ref[:, base + size : base + 2 * size]
        values = packed_ref[:, base + 2 * size : base + 3 * size]
        mixed_grad = mixed_grads[:, h * size : (h + 1) * size]
        probability = prob_ref[0, h]
        prob_grad = dot_nt(mixed_grad, values)
        inner = jnp.sum(probability * prob_grad, axis=-1, keepdims=True)
        score_grad = (probability * (prob_grad - inner) * scaling).astype(jnp.bfloat16)
        prob_low = probability.astype(jnp.bfloat16)
        q_grad = jnp.dot(score_grad, keys, preferred_element_type=jnp.float32)
        grad_ref[:, base : base + size] = q_grad.astype(jnp.bfloat16)
        grad_ref[:, base + size : base + 2 * size] = dot_tn(score_grad, queries).astype(jnp.bfloat16)
        grad_ref[:, base + 2 * size : base + 3 * size] = dot_tn(prob_low, mixed_grad).astype(jnp.bfloat16)
    part_ref[...] = dot_nt(qkv_ref[...], grad_ref[...]).astype(jnp.bfloat16)


def attend_back(packed, probability, vis_low, w_out, qkv_flat, size):
    rows, width = packed.shape
    images, heads = probability.shape[:2]
    return pl.pallas_call(
        lambda *refs: attend_back_kernel(size, *refs),
        grid=(images,),
        in_specs=[
            pl.BlockSpec((TILE, width), lambda i: (i, 0)),
            pl.BlockSpec((1, heads, TILE, TILE), lambda i: (i, 0, 0, 0)),
            pl.BlockSpec((vis_low.shape[0], TILE), lambda i: (0, i)),
            pl.BlockSpec(w_out.shape, lambda i: (0, 0)),
            pl.BlockSpec(qkv_flat.shape, lambda i: (0, 0)),
        ],
        out_specs=[
            pl.BlockSpec((TILE, width), lambda i: (i, 0)),
            pl.BlockSpec((vis_low.shape[0], TILE), lambda i: (0, i)),
        ],
        out_shape=[
            jax.ShapeDtypeStruct((rows, width), jnp.bfloat16),
            jax.ShapeDtypeStruct(vis_low.shape, jnp.bfloat16),
        ],
        cost_estimate=pl.CostEstimate(flops=3 * 10**9, bytes_accessed=6 * 10**6, transcendentals=0),
        name="attend_back",
    )(packed, probability, vis_low, w_out, qkv_flat)


def gathered(share, axis):
    total = lax.axis_size(axis)
    index = lax.axis_index(axis).astype(jnp.uint32)
    stacked = [share]
    for step in range(1, total):
        pairs = [(i, (i - step) % total) for i in range(total)]
        stacked.append(lax.ppermute(share, axis, pairs))
    twice = jnp.concatenate([part[None] for part in stacked + stacked[:-1]], axis=0)
    return lax.dynamic_slice_in_dim(twice, lax.rem(jnp.uint32(total) - index, jnp.uint32(total)), total, 0) if total > 1 else twice


def shards(grad_rows, features, block_in, patch_counts, owner, ln1_gain, w_qkv, w_out, w_proj):
    groups = lax.axis_size("enc")
    tp_size = lax.axis_size("tp")
    inner = inner_size(groups)
    device = lax.axis_index("enc")
    tp_rank = lax.axis_index("tp")
    block_rows = grad_rows.shape[0]
    img_group = block_rows // TILE
    share_width = block_in.shape[1]
    features_dim = features.shape[1]
    line_index = jnp.arange(TILE, dtype=jnp.int32)
    peer_index = jnp.arange(groups, dtype=jnp.int32)
    own_counts = lax.dynamic_index_in_dim(patch_counts, device, 0, keepdims=False)
    own_owner = lax.dynamic_index_in_dim(owner, device, 0, keepdims=False)
    live_own = line_index[None, :] < own_counts[:, None]

    sends = jnp.any(owner == device, axis=1)
    sends_int = sends.astype(jnp.int32)
    rank = jnp.cumsum(sends_int) - sends_int
    slot_index = jnp.arange(img_group, dtype=jnp.int32)
    source_of = jnp.sum(
        jnp.where(sends[None, :] & (rank[None, :] == slot_index[:, None]), peer_index[None, :], 0),
        axis=1,
    )
    source_owner = jnp.take(owner, source_of, axis=0)
    source_counts = jnp.take(patch_counts, source_of, axis=0)
    arrived_counts = jnp.sum(jnp.where(source_owner == device, source_counts, 0), axis=1)

    kept_rows = jnp.where(live_own.reshape(-1)[:, None], features, jnp.zeros_like(features))
    piece_rows = features_dim // groups
    grad_proj = summed_rows(kept_rows.T.reshape(groups, piece_rows, block_rows), grad_rows, "enc", inner, 2)

    vis_part = dot_nt(w_proj, grad_rows).astype(jnp.bfloat16)
    shared = two_stage_sum(vis_part.reshape(tp_size, share_width, block_rows), None, "tp", 2)
    tiles = jnp.where(live_own.reshape(-1)[None, :], shared, 0.0).astype(jnp.bfloat16)
    tiles = [tiles[:, j * TILE : (j + 1) * TILE] for j in range(img_group)]
    outgoing = jnp.zeros((groups, share_width, TILE), jnp.bfloat16)
    for j in range(img_group):
        outgoing = jnp.where((own_owner[j] == peer_index)[:, None, None], tiles[j][None], outgoing)
    received = lax.all_to_all(outgoing, "enc", split_axis=0, concat_axis=0, tiled=True)
    vis_share = jnp.concatenate([pick(received, source_of[j].astype(jnp.uint32), 0) for j in range(img_group)], axis=1)
    vis_low = gathered(vis_share, "tp").reshape(features_dim, block_rows)

    heads_here = w_qkv.shape[1]
    head_size = w_qkv.shape[2] // 3
    block_turned = block_in.T
    block_full = gathered(block_turned, "tp").reshape(features_dim, block_rows)
    qkv_flat = w_qkv.reshape(features_dim, heads_here * 3 * head_size)
    block_wide = block_full.astype(jnp.float32)
    centre = jnp.mean(block_wide, axis=0, keepdims=True)
    centred = block_wide - centre
    inverse1 = lax.rsqrt(jnp.mean(centred * centred, axis=0, keepdims=True) + EPSILON)
    normed_in = (centred * inverse1 * ln1_gain[:, None]).astype(jnp.bfloat16)
    packed = dot_tn(normed_in, qkv_flat).astype(jnp.bfloat16)
    probability, mixed = attend(packed, arrived_counts, heads_here, head_size)
    packed_grad, in_part = attend_back(packed, probability, vis_low, w_out, qkv_flat, head_size)

    in_sum = two_stage_sum(in_part.reshape(tp_size, share_width, block_rows), None, "tp", 2)
    normed_share = (block_turned.astype(jnp.float32) - centre) * inverse1
    gain_share = lax.dynamic_slice_in_dim(ln1_gain, tp_rank * share_width, share_width, 0)
    scaled = in_sum * gain_share[:, None]
    sums = jnp.concatenate([jnp.sum(scaled, axis=0), jnp.sum(scaled * normed_share, axis=0)])
    ln1_share = jnp.sum(in_sum * normed_share, axis=1)
    small = jnp.concatenate([sums, ln1_share])
    small = gathered(small, "tp")
    means = jnp.sum(small[:, : 2 * block_rows], axis=0).reshape(2, 1, block_rows) / features_dim
    in_back = inverse1 * (scaled - means[0] - normed_share * means[1])
    grad_input = (vis_share.astype(jnp.float32) + in_back).astype(jnp.bfloat16).T

    grad_qkv = summed_rows(
        normed_in.reshape(groups, piece_rows, block_rows), packed_grad, "enc", inner, 2
    ).reshape(piece_rows, heads_here, 3 * head_size)
    out_term = jnp.dot(vis_low, mixed, preferred_element_type=jnp.float32).astype(jnp.bfloat16)
    ln1_term = small[:, 2 * block_rows :].reshape(features_dim, 1).astype(jnp.bfloat16)
    both = jnp.concatenate([out_term, ln1_term], axis=1)
    both = two_stage_sum(both.reshape(groups, piece_rows, -1), None, "enc", inner)
    grad_out = both[:, :-1].T
    grad_ln1 = both[:, -1]
    return (grad_input, grad_proj, grad_qkv, grad_out, grad_ln1)


def solution(mesh):
    placed = (
        P("enc", "tp"),
        P("enc", None),
        P("enc", "tp"),
        P(),
        P(),
        P(),
        P(None, "tp", None),
        P("tp", None),
        P(None, "tp"),
    )
    return jax.shard_map(
        shards,
        mesh=mesh,
        in_specs=placed,
        out_specs=(P("enc", "tp"), P("enc", "tp"), P("enc", "tp", None), P("tp", "enc"), P("enc")),
        check_vma=False,
    )
```

```python
import jax
import jax.numpy as jnp
from jax import lax
from jax.experimental import pallas as pl
from jax.experimental.pallas import tpu as pltpu
from jax.sharding import PartitionSpec as P


TILE = 128


EPSILON = 1e-05


def dot_nt(left, right):
    return lax.dot_general(
        left, right, (((1,), (1,)), ((), ())), preferred_element_type=jnp.float32
    )


def dot_tn(left, right):
    return lax.dot_general(
        left, right, (((0,), (0,)), ((), ())), preferred_element_type=jnp.float32
    )


def inner_size(groups):
    inner = 1
    while inner * inner * 4 <= groups:
        inner *= 2
    return inner


def pick(values, place, dim):
    return lax.dynamic_index_in_dim(values, place, dim, keepdims=False, allow_negative_indices=False)


def two_stage_sum(left, right, axis, inner):
    total = left.shape[0]
    outer = total // inner
    index = lax.axis_index(axis).astype(jnp.uint32)
    at_outer, at_inner = lax.div(index, jnp.uint32(inner)), lax.rem(index, jnp.uint32(inner))
    lefts = left.reshape((outer, inner) + left.shape[1:])

    def term(place):
        chosen = pick(lefts, place, 1)
        if right is None:
            return chosen
        flat = chosen.reshape(-1, chosen.shape[-1])
        product = jnp.dot(flat, right, preferred_element_type=jnp.float32).astype(jnp.bfloat16)
        return product.reshape(outer, -1, right.shape[1])

    arrived = []
    for step in range(1, inner):
        pairs = [(o * inner + i, o * inner + (i + step) % inner) for o in range(outer) for i in range(inner)]
        sent = term(lax.rem(at_inner + jnp.uint32(step), jnp.uint32(inner)))
        arrived.append(lax.ppermute(sent, axis, pairs))
    running = term(at_inner).astype(jnp.float32)
    for value in arrived:
        running += value.astype(jnp.float32)
    summed = pick(running, at_outer, 0)
    short = running.astype(jnp.bfloat16)
    arrived = []
    for step in range(1, outer):
        pairs = [(o * inner + i, (o + step) % outer * inner + i) for o in range(outer) for i in range(inner)]
        sent = pick(short, lax.rem(at_outer + jnp.uint32(step), jnp.uint32(outer)), 0)
        arrived.append(lax.ppermute(sent, axis, pairs))
    for value in arrived:
        summed += value.astype(jnp.float32)
    return summed


def summed_rows(left, right, axis, inner, cuts):
    rows = left.shape[1]
    if rows % (16 * cuts):
        cuts = 1
    height = rows // cuts
    pieces = [two_stage_sum(left[:, c * height : (c + 1) * height], right, axis, inner) for c in range(cuts)]
    return jnp.concatenate(pieces, axis=0) if cuts > 1 else pieces[0]


def attend_kernel(size, counts_ref, packed_ref, prob_ref, mixed_ref):
    tile = packed_ref.shape[0]
    count = counts_ref[pl.program_id(0)]
    rows = lax.broadcasted_iota(jnp.int32, (tile, tile), 0) < count
    columns = lax.broadcasted_iota(jnp.int32, (tile, tile), 1) < count
    same = jnp.logical_not(jnp.logical_xor(rows, columns))
    scaling = 1.0 / size**0.5
    for h in range(prob_ref.shape[1]):
        base = h * 3 * size
        queries = packed_ref[:, base : base + size]
        keys = packed_ref[:, base + size : base + 2 * size]
        values = packed_ref[:, base + 2 * size : base + 3 * size]
        scores = jnp.where(same, dot_nt(queries, keys) * scaling, -1e30)
        terms = jnp.exp(scores - jnp.max(scores, axis=-1, keepdims=True))
        probability = terms / jnp.sum(terms, axis=-1, keepdims=True)
        prob_ref[0, h] = probability
        mixed = jnp.dot(probability.astype(jnp.bfloat16), values, preferred_element_type=jnp.float32)
        mixed_ref[:, h * size : (h + 1) * size] = mixed.astype(jnp.bfloat16)


def attend(packed, counts, heads, size):
    rows = packed.shape[0]
    images = rows // TILE
    return pl.pallas_call(
        lambda *refs: attend_kernel(size, *refs),
        grid=(images,),
        in_specs=[
            pl.BlockSpec(memory_space=pltpu.SMEM),
            pl.BlockSpec((TILE, packed.shape[1]), lambda i: (i, 0)),
        ],
        out_specs=[
            pl.BlockSpec((1, heads, TILE, TILE), lambda i: (i, 0, 0, 0)),
            pl.BlockSpec((TILE, heads * size), lambda i: (i, 0)),
        ],
        out_shape=[
            jax.ShapeDtypeStruct((images, heads, TILE, TILE), jnp.float32),
            jax.ShapeDtypeStruct((rows, heads * size), jnp.bfloat16),
        ],
        cost_estimate=pl.CostEstimate(flops=2 * 10**9, bytes_accessed=4 * 10**6, transcendentals=0),
        name="attend",
    )(counts, packed)


def attend_back_kernel(size, packed_ref, prob_ref, vis_ref, out_ref, qkv_ref, grad_ref, part_ref):
    scaling = 1.0 / size**0.5
    mixed_grads = lax.dot_general(
        vis_ref[...], out_ref[...], (((0,), (1,)), ((), ())), preferred_element_type=jnp.float32
    ).astype(jnp.bfloat16)
    for h in range(prob_ref.shape[1]):
        base = h * 3 * size
        queries = packed_ref[:, base : base + size]
        keys = packed_ref[:, base + size : base + 2 * size]
        values = packed_ref[:, base + 2 * size : base + 3 * size]
        mixed_grad = mixed_grads[:, h * size : (h + 1) * size]
        probability = prob_ref[0, h]
        prob_grad = dot_nt(mixed_grad, values)
        inner = jnp.sum(probability * prob_grad, axis=-1, keepdims=True)
        score_grad = (probability * (prob_grad - inner) * scaling).astype(jnp.bfloat16)
        prob_low = probability.astype(jnp.bfloat16)
        q_grad = jnp.dot(score_grad, keys, preferred_element_type=jnp.float32)
        grad_ref[:, base : base + size] = q_grad.astype(jnp.bfloat16)
        grad_ref[:, base + size : base + 2 * size] = dot_tn(score_grad, queries).astype(jnp.bfloat16)
        grad_ref[:, base + 2 * size : base + 3 * size] = dot_tn(prob_low, mixed_grad).astype(jnp.bfloat16)
    part_ref[...] = dot_nt(qkv_ref[...], grad_ref[...]).astype(jnp.bfloat16)


def attend_back(packed, probability, vis_low, w_out, qkv_flat, size):
    rows, width = packed.shape
    images, heads = probability.shape[:2]
    return pl.pallas_call(
        lambda *refs: attend_back_kernel(size, *refs),
        grid=(images,),
        in_specs=[
            pl.BlockSpec((TILE, width), lambda i: (i, 0)),
            pl.BlockSpec((1, heads, TILE, TILE), lambda i: (i, 0, 0, 0)),
            pl.BlockSpec((vis_low.shape[0], TILE), lambda i: (0, i)),
            pl.BlockSpec(w_out.shape, lambda i: (0, 0)),
            pl.BlockSpec(qkv_flat.shape, lambda i: (0, 0)),
        ],
        out_specs=[
            pl.BlockSpec((TILE, width), lambda i: (i, 0)),
            pl.BlockSpec((vis_low.shape[0], TILE), lambda i: (0, i)),
        ],
        out_shape=[
            jax.ShapeDtypeStruct((rows, width), jnp.bfloat16),
            jax.ShapeDtypeStruct(vis_low.shape, jnp.bfloat16),
        ],
        cost_estimate=pl.CostEstimate(flops=3 * 10**9, bytes_accessed=6 * 10**6, transcendentals=0),
        name="attend_back",
    )(packed, probability, vis_low, w_out, qkv_flat)


def gathered(share, axis):
    total = lax.axis_size(axis)
    index = lax.axis_index(axis).astype(jnp.uint32)
    stacked = [share]
    for step in range(1, total):
        pairs = [(i, (i - step) % total) for i in range(total)]
        stacked.append(lax.ppermute(share, axis, pairs))
    twice = jnp.concatenate([part[None] for part in stacked + stacked[:-1]], axis=0)
    return lax.dynamic_slice_in_dim(twice, lax.rem(jnp.uint32(total) - index, jnp.uint32(total)), total, 0) if total > 1 else twice


def shards(grad_rows, features, block_in, patch_counts, owner, ln1_gain, w_qkv, w_out, w_proj):
    groups = lax.axis_size("enc")
    tp_size = lax.axis_size("tp")
    inner = inner_size(groups)
    device = lax.axis_index("enc")
    tp_rank = lax.axis_index("tp")
    block_rows = grad_rows.shape[0]
    img_group = block_rows // TILE
    share_width = block_in.shape[1]
    features_dim = features.shape[1]
    line_index = jnp.arange(TILE, dtype=jnp.int32)
    peer_index = jnp.arange(groups, dtype=jnp.int32)
    own_counts = lax.dynamic_index_in_dim(patch_counts, device, 0, keepdims=False)
    own_owner = lax.dynamic_index_in_dim(owner, device, 0, keepdims=False)
    live_own = line_index[None, :] < own_counts[:, None]

    sends = jnp.any(owner == device, axis=1)
    sends_int = sends.astype(jnp.int32)
    rank = jnp.cumsum(sends_int) - sends_int
    slot_index = jnp.arange(img_group, dtype=jnp.int32)
    source_of = jnp.sum(
        jnp.where(sends[None, :] & (rank[None, :] == slot_index[:, None]), peer_index[None, :], 0),
        axis=1,
    )
    source_owner = jnp.take(owner, source_of, axis=0)
    source_counts = jnp.take(patch_counts, source_of, axis=0)
    arrived_counts = jnp.sum(jnp.where(source_owner == device, source_counts, 0), axis=1)

    kept_rows = jnp.where(live_own.reshape(-1)[:, None], features, jnp.zeros_like(features))
    piece_rows = features_dim // groups
    grad_proj = summed_rows(kept_rows.T.reshape(groups, piece_rows, block_rows), grad_rows, "enc", inner, 2)

    vis_part = dot_nt(w_proj, grad_rows).astype(jnp.bfloat16)
    shared = two_stage_sum(vis_part.reshape(tp_size, share_width, block_rows), None, "tp", 2)
    tiles = jnp.where(live_own.reshape(-1)[None, :], shared, 0.0).astype(jnp.bfloat16)
    tiles = [tiles[:, j * TILE : (j + 1) * TILE] for j in range(img_group)]
    outgoing = jnp.zeros((groups, share_width, TILE), jnp.bfloat16)
    for j in range(img_group):
        outgoing = jnp.where((own_owner[j] == peer_index)[:, None, None], tiles[j][None], outgoing)
    received = lax.all_to_all(outgoing, "enc", split_axis=0, concat_axis=0, tiled=True)
    vis_share = jnp.concatenate([pick(received, source_of[j].astype(jnp.uint32), 0) for j in range(img_group)], axis=1)
    vis_low = gathered(vis_share, "tp").reshape(features_dim, block_rows)

    heads_here = w_qkv.shape[1]
    head_size = w_qkv.shape[2] // 3
    block_turned = block_in.T
    block_full = gathered(block_turned, "tp").reshape(features_dim, block_rows)
    qkv_flat = w_qkv.reshape(features_dim, heads_here * 3 * head_size)
    block_wide = block_full.astype(jnp.float32)
    centre = jnp.mean(block_wide, axis=0, keepdims=True)
    centred = block_wide - centre
    inverse1 = lax.rsqrt(jnp.mean(centred * centred, axis=0, keepdims=True) + EPSILON)
    normed_in = (centred * inverse1 * ln1_gain[:, None]).astype(jnp.bfloat16)
    packed = dot_tn(normed_in, qkv_flat).astype(jnp.bfloat16)
    probability, mixed = attend(packed, arrived_counts, heads_here, head_size)
    packed_grad, in_part = attend_back(packed, probability, vis_low, w_out, qkv_flat, head_size)

    in_sum = two_stage_sum(in_part.reshape(tp_size, share_width, block_rows), None, "tp", 2)
    normed_share = (block_turned.astype(jnp.float32) - centre) * inverse1
    gain_share = lax.dynamic_slice_in_dim(ln1_gain, tp_rank * share_width, share_width, 0)
    scaled = in_sum * gain_share[:, None]
    sums = jnp.concatenate([jnp.sum(scaled, axis=0), jnp.sum(scaled * normed_share, axis=0)])
    ln1_share = jnp.sum(in_sum * normed_share, axis=1)
    small = jnp.concatenate([sums, ln1_share])
    small = gathered(small, "tp")
    means = jnp.sum(small[:, : 2 * block_rows], axis=0).reshape(2, 1, block_rows) / features_dim
    in_back = inverse1 * (scaled - means[0] - normed_share * means[1])
    grad_input = (vis_share.astype(jnp.float32) + in_back).astype(jnp.bfloat16).T

    grad_qkv = summed_rows(
        normed_in.reshape(groups, piece_rows, block_rows), packed_grad, "enc", inner, 2
    ).reshape(piece_rows, heads_here, 3 * head_size)
    out_term = jnp.dot(vis_low, mixed, preferred_element_type=jnp.float32).astype(jnp.bfloat16)
    grad_out = two_stage_sum(out_term.reshape(groups, piece_rows, -1), None, "enc", inner).T
    ln1_term = small[:, 2 * block_rows :].reshape(groups, piece_rows).astype(jnp.bfloat16)
    grad_ln1 = two_stage_sum(ln1_term, None, "enc", inner)
    return (grad_input, grad_proj, grad_qkv, grad_out, grad_ln1)


def solution(mesh):
    placed = (
        P("enc", "tp"),
        P("enc", None),
        P("enc", "tp"),
        P(),
        P(),
        P(),
        P(None, "tp", None),
        P("tp", None),
        P(None, "tp"),
    )
    return jax.shard_map(
        shards,
        mesh=mesh,
        in_specs=placed,
        out_specs=(P("enc", "tp"), P("enc", "tp"), P("enc", "tp", None), P("tp", "enc"), P("enc")),
        check_vma=False,
    )
```
